256 devices in a mesh: section: 4 (over x), tensor: 16 (over z, core), dp: 4 (over y).
Axes of the slice: x: 4, y: 4, z: 8, core: 2. Of those that a mesh axis runs over, the one named last changes fastest.
Arguments:
- hidden_in: bfloat16 [128, 4096], P('dp', 'tensor'), may hold values from -6 to 6
- norm_gain: float32 [4, 4096], P('section'), may hold values from 0.25 to 1.75
- gate_weight: bfloat16 [4, 4096, 8192], P('section', 'dp', 'tensor'), may hold values from -0.09375 to 0.09375
- up_weight: bfloat16 [4, 4096, 8192], P('section', 'dp', 'tensor'), may hold values from -0.09375 to 0.09375
- down_weight: bfloat16 [4, 4096, 8192], P('section', 'dp', 'tensor'), may hold values from -0.0625 to 0.0625
- lengths: int32 [16], P('dp'), may hold values from 3 to 8
Outputs:
- rdm: float32 [4, 16, 16], P('section', 'dp')
The draws below stay inside these ranges and needn't reach their ends.
Inputs may be any that keep to these rules, and one draw needn't show every extreme that they name: `lengths`: the number of leading valid token rows of each sentence.
All inputs are finite; a program needn't handle non-finite values.
Results may differ from the reference program's by a relative error of at most 0.0012.
Values may be sent and summed in bfloat16 or wider, within the bound.
A program may use at most 128 MiB of HBM per device.

```python
import jax
import jax.numpy as jnp
from jax import lax

D = 4096
FF = 8192
LEN = 8
SENT = 16
TOKENS = 128
SECTIONS = 4
N_SECTION = 4


def plant(drawn, own_key, smallest, top_value):
    longest = drawn.shape.index(max(drawn.shape))
    spots = []
    for shift in (0, 1):
        where = [jax.random.randint(jax.random.fold_in(own_key, axis), (), 0, length) for axis, length in enumerate(drawn.shape)]
        where[longest] = (where[longest] + shift) % drawn.shape[longest]
        spots.append(tuple(where))
    return drawn.at[spots[0]].set(smallest).at[spots[1]].set(top_value)


def block_scale(own_key, shape, pieces, least, largest):
    loudness, own = 1.0, jax.random.fold_in(own_key, 6)
    for axis_at, parts in pieces:
        draws = jnp.exp(jax.random.uniform(jax.random.fold_in(own, axis_at), (parts,), jnp.float32, least / len(pieces), largest / len(pieces)))
        loudness = loudness * jnp.repeat(draws, shape[axis_at] // parts).reshape([-1 if axis == axis_at else 1 for axis in range(len(shape))])
    return loudness


def gaussian(stream_key, dims, deviation, most, split=(), kind=jnp.bfloat16):
    values = deviation * jax.random.normal(stream_key, dims, jnp.float32)
    if split:
        values = values * block_scale(stream_key, dims, split, -0.22, 0.18)
    return jnp.clip(values, -most, most).astype(kind)


def setup_inputs(seed: int = 0) -> dict:
    keys = jax.random.split(jax.random.key(seed), 7)
    return {
        "hidden_in": gaussian(keys[0], (TOKENS, D), 1.0, 6.0, ((0, 4), (1, 16))),
        "norm_gain": jnp.clip(1.0 + 0.15 * jax.random.normal(keys[1], (SECTIONS, D), jnp.float32), 0.25, 1.75),
        "gate_weight": gaussian(keys[2], (SECTIONS, D, FF), D ** -0.5, 0.09375, ((0, 4), (1, 4), (2, 16))),
        "up_weight": gaussian(keys[3], (SECTIONS, D, FF), D ** -0.5, 0.09375, ((0, 4), (1, 4), (2, 16))),
        "down_weight": gaussian(keys[4], (SECTIONS, D, FF), FF ** -0.5, 0.0625, ((0, 4), (1, 4), (2, 16))),
        "lengths": plant(jax.random.randint(keys[5], (SENT,), 3, LEN + 1), jax.random.fold_in(keys[5], 1), 3, LEN).astype(jnp.int32),
    }


RMS_EPS = 1e-05
UNIT_FLOOR = 0.1
CONTRACT_LAST = (((1,), (1,)), ((), ()))

def reference(hidden_in, norm_gain, gate_weight, up_weight, down_weight, lengths):
    current = hidden_in
    positions = jnp.arange(LEN, dtype=jnp.int32)
    weights = (positions[None, :] < lengths[:, None]).astype(jnp.float32)
    counts = lengths.astype(jnp.float32)
    results = []
    for layer in range(N_SECTION):
        wide_state = current.astype(jnp.float32)
        inv_rms = lax.rsqrt(lax.optimization_barrier(jnp.mean(wide_state * wide_state, axis=1, keepdims=True)) + RMS_EPS)
        normed = (wide_state * inv_rms * norm_gain[layer][None, :]).astype(jnp.bfloat16)
        gate_sum = jnp.dot(normed, gate_weight[layer], preferred_element_type=jnp.float32)
        up_sum = jnp.dot(normed, up_weight[layer], preferred_element_type=jnp.float32)
        hidden = (jax.nn.silu(gate_sum) * up_sum).astype(jnp.bfloat16)
        summed = lax.dot_general(hidden, down_weight[layer], CONTRACT_LAST, preferred_element_type=jnp.float32)
        current = (wide_state + summed).astype(jnp.bfloat16)
        shaped = current.astype(jnp.float32).reshape(SENT, LEN, D)
        pooled = lax.optimization_barrier(jnp.sum(shaped * weights[:, :, None], axis=1)) / counts[:, None]
        centered = pooled - lax.optimization_barrier(jnp.mean(pooled, axis=1, keepdims=True))
        unit_rows = (centered * lax.rsqrt(lax.optimization_barrier(jnp.mean(centered * centered, axis=1, keepdims=True)) + UNIT_FLOOR)).astype(jnp.bfloat16)
        products = lax.dot_general(unit_rows, unit_rows, CONTRACT_LAST, preferred_element_type=jnp.float32)
        results.append(1.0 - products / D)
    return jnp.stack(results)
```

```python
import jax
import jax.numpy as jnp
from jax import lax
from jax.experimental import pallas as pl
from jax.experimental.pallas import tpu as pltpu
from jax.sharding import PartitionSpec as P

D = 4096
LEN = 8
SENT = 16
NY = 4
NZ = 8
NS = 4
ROWS = D // NY
FFC = 1024
SUB = FFC // NY
COL = ROWS // NZ
GROUP = 64
K = 2
T = GROUP // K
SPC = T // LEN
PARTS = 32 // T
RMS_EPS = 1e-05
UNIT_FLOOR = 0.1
NT = (((1,), (1,)), ((), ()))
MESH = pl.DeviceIdType.MESH
F32 = jnp.float32
BF16 = jnp.bfloat16


def kernel(
    hid_in, gain_in, gate_in, up_in, down_in, len_in, out_ref,
    hv, gv, wg, wu, wd, xb, ps, pr, sr, hr, zs, zr, yo, wl, pv, gz, gy, fs,
    in_sem, w_sem, wsend, wrecv, dsend, xsem, psend, prsem, ssend, srsem,
    hsend, hrsem, zsend, zrsem, ysend, lsend, lrsem, csend, crsem, gzsend, gzsem, gysend, gysem,
):
    s = lax.axis_index("section")
    t = lax.axis_index("tensor")
    y = lax.axis_index("dp")
    z = t // 2
    c = t % 2

    def at(sec, zz, cc, yy):
        return {"section": sec, "tensor": zz * 2 + cc, "dp": yy}

    def remote(src, dst, ssem, rsem, dev):
        return pltpu.make_async_remote_copy(
            src_ref=src, dst_ref=dst, send_sem=ssem, recv_sem=rsem, device_id=dev, device_id_type=MESH
        )

    me = at(s, z, c, y)

    hid_cp = pltpu.make_async_copy(hid_in, hv, in_sem.at[0])
    hid_cp.start()
    gain_cp = pltpu.make_async_copy(
        gain_in.at[:, pl.ds(pl.multiple_of(y * ROWS, ROWS), ROWS)], gv, in_sem.at[1]
    )
    loads = []
    for i in range(2):
        loads.append(pltpu.make_async_copy(gate_in.at[0, :, pl.ds(SUB * i, SUB)], wg.at[2 * c + i], w_sem.at[i]))
        loads.append(pltpu.make_async_copy(up_in.at[0, :, pl.ds(SUB * i, SUB)], wu.at[2 * c + i], w_sem.at[2 + i]))
    loads.append(pltpu.make_async_copy(down_in, wd.at[c], w_sem.at[4]))
    for cp in loads:
        cp.start()
    gain_cp.start()

    barrier = pltpu.get_barrier_semaphore()

    def greet(dev):
        pl.semaphore_signal(barrier, inc=1, device_id=dev, device_id_type=MESH)

    first = s == 0
    last = s == NS - 1
    src_y = 2 * c
    self_feed = jnp.logical_and(y == z // 2, c == y // 2)

    @pl.when(first)
    def _():
        def feed_greet(i, carry):
            @pl.when(jnp.logical_not(jnp.logical_and(self_feed, i == z)))
            def _():
                greet(at(s, i, y // 2, z // 2))

            sy = src_y + i // 4
            sz = 2 * y + (i // 2) % 2
            sc = i % 2

            @pl.when(jnp.logical_not(jnp.logical_and(sy == y, jnp.logical_and(sz == z, sc == c))))
            def _():
                greet(at(s, sz, sc, sy))

            return carry

        lax.fori_loop(0, NZ, feed_greet, 0)

    def z_greet(i, carry):
        @pl.when(i > 0)
        def _():
            greet(at(s, (z + i) % NZ, c, y))

        @pl.when(s > 0)
        def _():
            greet(at(s - 1, (z + i) % NZ, c, y))

        @pl.when(s < NS - 1)
        def _():
            greet(at(s + 1, (z + i) % NZ, c, y))

        return carry

    lax.fori_loop(0, NZ, z_greet, 0)
    for d in range(1, NY):
        greet(at(s, z, c, (y + d) % NY))
    greet(at(s, z, 1 - c, y))
    own_feed = jnp.where(self_feed, 1, 0)
    peers = 1 + (NY - 1) + (NZ - 1)
    peers = peers + jnp.where(s > 0, NZ, 0) + jnp.where(s < NS - 1, NZ, 0)
    peers = peers + jnp.where(first, 2 * NZ - 2 * own_feed, 0)

    pos = lax.broadcasted_iota(jnp.int32, (LEN, 128), 0)
    for i in range(SENT // NY):
        n = len_in[i]
        wl[y * (SENT // NY) + i] = jnp.where(pos < n, 1.0 / jnp.full((LEN, 128), n, jnp.int32).astype(F32), 0.0)

    hid_cp.wait()
    pl.semaphore_wait(barrier, peers)

    @pl.when(first)
    def _():
        def feed(i, carry):
            zz = (z + NZ // 2 + i) % NZ
            for q in range(PARTS):
                for h in range(2):
                    src = hv.at[pl.ds(q * T, T), pl.ds(COL * h, COL)]
                    k = (y % 2) * PARTS + q
                    j = (z % 2) * 4 + c * 2 + h
                    dst = xb.at[k, j]
                    n = q * 2 + h

                    @pl.when(jnp.logical_and(self_feed, zz == z))
                    def _():
                        pltpu.make_async_copy(src, dst, xsem.at[k, j]).start()

                    @pl.when(jnp.logical_not(jnp.logical_and(self_feed, zz == z)))
                    def _():
                        remote(src, dst, dsend.at[i, n], xsem.at[k, j], at(s, zz, y // 2, z // 2)).start()

            return carry

        lax.fori_loop(0, NZ, feed, 0)

    for cp in loads:
        cp.wait()
    partner = at(s, z, 1 - c, y)
    swaps = [
        remote(wg.at[pl.ds(2 * c, 2)], wg.at[pl.ds(2 * c, 2)], wsend.at[0], wrecv.at[0], partner),
        remote(wu.at[pl.ds(2 * c, 2)], wu.at[pl.ds(2 * c, 2)], wsend.at[1], wrecv.at[1], partner),
        remote(wd.at[c], wd.at[c], wsend.at[2], wrecv.at[2], partner),
    ]
    for cp in swaps:
        cp.start()

    mine = wl.at[pl.ds(y * (SENT // NY), SENT // NY)]
    for d in range(1, NY):
        remote(mine, mine, lsend.at[d], lrsem.at[y], at(s, z, c, (y + d) % NY)).start()

    gain_cp.wait()
    swaps[0].wait_recv()
    swaps[1].wait_recv()

    lane_t = lax.broadcasted_iota(jnp.int32, (T, 128), 1)
    row_t = lax.broadcasted_iota(jnp.int32, (T, 128), 0)
    eye_t = lane_t == row_t

    def stage1(k):
        for j in range(NZ):
            remote(xb.at[k, j], xb.at[k, j], dsend.at[0, 0], xsem.at[k, j], me).wait_recv()
        x = jnp.concatenate([xb[k, j] for j in range(NZ)], axis=1).astype(F32)
        square = jnp.sum(x * x, axis=1, keepdims=True)
        sr[k, y] = jnp.sum(jnp.where(eye_t, square, 0.0), axis=0, keepdims=True)
        xg = (x * gv[...]).astype(BF16)
        for n, d in enumerate((2, 1, 3, 0)):
            yb = (y + d) % NY
            gate = jnp.dot(xg, wg[yb], preferred_element_type=F32)
            up = jnp.dot(xg, wu[yb], preferred_element_type=F32)
            both = jnp.concatenate([gate, up], axis=1).astype(BF16)
            if d == 0:
                pr[k, y] = both
            else:
                ps[k, d - 1] = both
                dev = at(s, z, c, yb)
                remote(sr.at[k, y], sr.at[k, y], ssend.at[k, d], srsem.at[k, y], dev).start()
                remote(ps.at[k, d - 1], pr.at[k, y], psend.at[k, d], prsem.at[k, y], dev).start()

    def stage2(k):
        for d in range(1, NY):
            src = (y + d) % NY
            remote(sr.at[k, src], sr.at[k, src], ssend.at[k, d], srsem.at[k, src], me).wait_recv()
            remote(pr.at[k, src], pr.at[k, src], psend.at[k, d], prsem.at[k, src], me).wait_recv()
        row = sr[k, 0] + sr[k, 1] + sr[k, 2] + sr[k, 3]
        square = jnp.sum(jnp.where(eye_t, row, 0.0), axis=1, keepdims=True)
        inv = lax.rsqrt(square * (1.0 / D) + RMS_EPS)
        total = pr[k, 0].astype(F32) + pr[k, 1].astype(F32) + pr[k, 2].astype(F32) + pr[k, 3].astype(F32)
        total = total * inv
        gate = total[:, :SUB]
        up = total[:, SUB:]
        hr[k, y] = (gate / (1.0 + jnp.exp(-gate)) * up).astype(BF16)
        for d in (2, 1, 3):
            remote(hr.at[k, y], hr.at[k, y], hsend.at[k, d], hrsem.at[k, y], at(s, z, c, (y + d) % NY)).start()

    def stage3(k):
        for d in range(1, NY):
            src = (y + d) % NY
            remote(hr.at[k, src], hr.at[k, src], hsend.at[k, d], hrsem.at[k, src], me).wait_recv()
        left = jnp.concatenate([hr[k, 0], hr[k, 1]], axis=1)
        right = jnp.concatenate([hr[k, 2], hr[k, 3]], axis=1)
        for d in (2, 1, 3, 0):
            p = (z // 2 + d) % 4
            part = lax.dot_general(left, wd[0, p], NT, preferred_element_type=F32)
            part += lax.dot_general(right, wd[1, p], NT, preferred_element_type=F32)
            part = part.astype(BF16)
            for i in range(2):
                j = 2 * p + i
                piece = part[:, COL * i : COL * (i + 1)]

                def send():
                    zs[k, j] = piece
                    remote(zs.at[k, j], zr.at[k, z], zsend.at[k, j], zrsem.at[k, z], at(s, j, c, y)).start()

                if d != 0:
                    send()
                else:

                    @pl.when(j == z)
                    def _():
                        zr[k, z] = piece

                    pl.when(j != z)(send)

    def stage4(k):
        for d in range(1, NZ):
            src = (z + d) % NZ
            remote(zr.at[k, src], zr.at[k, src], zsend.at[k, 0], zrsem.at[k, src], me).wait_recv()
        total = xb[k, z].astype(F32)
        for j in range(NZ):
            total += zr[k, j].astype(F32)
        state = total.astype(BF16)
        yo[k] = state

        @pl.when(s < NS - 1)
        def _():
            for d in (4, 3, 5, 2, 6, 1, 7, 0):
                zz = (z + d) % NZ
                remote(yo.at[k], xb.at[k, z], ysend.at[k, d], xsem.at[k, z], at(s + 1, zz, c, y)).start()

        weights = wl[pl.ds(c * (SENT // 2) + k * SPC, SPC)]
        pooled = jnp.sum(state.astype(F32).reshape(SPC, LEN, COL) * weights, axis=1)
        pv[c, pl.ds(k * SPC, SPC), :] = pooled

    for k in range(K):
        stage1(k)
    for k in range(K):
        stage2(k)
    swaps[2].wait_recv()
    for k in range(K):
        stage3(k)
    for d in range(1, NY):
        src = (y + d) % NY
        theirs = wl.at[pl.ds(src * (SENT // NY), SENT // NY)]
        remote(theirs, theirs, lsend.at[d], lrsem.at[src], me).wait_recv()
    for k in range(K):
        stage4(k)

    remote(pv.at[c], pv.at[c], csend, crsem, partner).start()
    remote(pv.at[1 - c], pv.at[1 - c], csend, crsem, partner).wait_recv()
    points = jnp.concatenate([pv[0], pv[1]], axis=0)
    mean = jnp.mean(points, axis=1, keepdims=True)
    points = points - mean
    padded = jnp.concatenate([points, jnp.zeros((128 - SENT, COL), F32)], axis=0)
    gram = lax.dot_general(points, padded, NT, precision=lax.Precision.HIGHEST, preferred_element_type=F32)
    lane = lax.broadcasted_iota(jnp.int32, (SENT, 128), 1)
    rowi = lax.broadcasted_iota(jnp.int32, (SENT, 128), 0)
    gz[z] = gram + jnp.where(lane == 32 + y * NZ + z, mean, 0.0)
    for d in (4, 3, 5, 2, 6, 1, 7):
        remote(gz.at[z], gz.at[z], gzsend.at[d], gzsem.at[z], at(s, (z + d) % NZ, c, y)).start()
    for d in range(1, NZ):
        src = (z + d) % NZ
        remote(gz.at[src], gz.at[src], gzsend.at[d], gzsem.at[src], me).wait_recv()
    sums = gz[0]
    for j in range(1, NZ):
        sums += gz[j]
    gy[y] = sums
    for d in (2, 1, 3):
        remote(gy.at[y], gy.at[y], gysend.at[d], gysem.at[y], at(s, z, c, (y + d) % NY)).start()
    for d in range(1, NY):
        src = (y + d) % NY
        remote(gy.at[src], gy.at[src], gysend.at[d], gysem.at[src], me).wait_recv()
    sums = gy[0] + gy[1] + gy[2] + gy[3]
    blocks = NY * NZ
    held = jnp.logical_and(lane >= 32, lane < 32 + blocks)
    means = jnp.where(held, sums, 0.0)
    means = jnp.where(held, means - jnp.sum(means, axis=1, keepdims=True) * (1.0 / blocks), 0.0)
    means_padded = jnp.concatenate([means, jnp.zeros((128 - SENT, 128), F32)], axis=0)
    cross = lax.dot_general(means, means_padded, NT, precision=lax.Precision.HIGHEST, preferred_element_type=F32)
    cov = (sums + COL * cross) * (1.0 / D)
    eye = lane == rowi
    scale = lax.rsqrt(jnp.sum(jnp.where(eye, cov, 0.0), axis=1, keepdims=True) + UNIT_FLOOR)
    scale_row = jnp.sum(jnp.where(eye, scale, 0.0), axis=0, keepdims=True)
    rdm = 1.0 - cov * scale * scale_row
    for i in range(NY):
        fs[i] = rdm[4 * i : 4 * i + 4]
    out_ref[0] = fs[y][:, :SENT]

    def sent(ref, sem):
        remote(ref, ref, sem, sem, partner).wait_send()

    @pl.when(first)
    def _():
        def drain(i, carry):
            zz = (z + NZ // 2 + i) % NZ

            for q in range(PARTS):
                for h in range(2):

                    @pl.when(jnp.logical_not(jnp.logical_and(self_feed, zz == z)))
                    def _():
                        sent(hv.at[pl.ds(q * T, T), pl.ds(COL * h, COL)], dsend.at[i, q * 2 + h])

            return carry

        lax.fori_loop(0, NZ, drain, 0)

    for cp in swaps:
        cp.wait_send()
    for d in range(1, NY):
        sent(mine, lsend.at[d])
        sent(gy.at[y], gysend.at[d])
    for d in range(1, NZ):
        sent(gz.at[z], gzsend.at[d])
    sent(pv.at[c], csend)

    def drain_chunk(k, carry):
        for d in range(1, NY):
            sent(sr.at[k, y], ssend.at[k, d])
            sent(ps.at[k, d - 1], psend.at[k, d])
            sent(hr.at[k, y], hsend.at[k, d])
        for j in range(NZ):

            @pl.when(j != z)
            def _():
                sent(zs.at[k, j], zsend.at[k, j])

        @pl.when(s < NS - 1)
        def _():
            for d in range(NZ):
                sent(yo.at[k], ysend.at[k, d])

        return carry

    lax.fori_loop(0, K, drain_chunk, 0)


def per_device(hidden_in, norm_gain, gate_weight, up_weight, down_weight, lengths):
    down = down_weight.reshape(4, 256, down_weight.shape[2])
    dma = pltpu.SemaphoreType.DMA
    any_space = pl.BlockSpec(memory_space=pl.ANY)
    return pl.pallas_call(
        kernel,
        out_shape=jax.ShapeDtypeStruct((1, SENT // NY, SENT), F32),
        in_specs=[any_space] * 5 + [pl.BlockSpec(memory_space=pltpu.SMEM)],
        out_specs=pl.BlockSpec(memory_space=pltpu.VMEM),
        scratch_shapes=[
            pltpu.VMEM((32, 256), BF16),
            pltpu.VMEM((1, ROWS), F32),
            pltpu.VMEM((NY, ROWS, SUB), BF16),
            pltpu.VMEM((NY, ROWS, SUB), BF16),
            pltpu.VMEM((2, 4, 256, 512), BF16),
            pltpu.VMEM((K, NZ, T, COL), BF16),
            pltpu.VMEM((K, NY - 1, T, 2 * SUB), BF16),
            pltpu.VMEM((K, NY, T, 2 * SUB), BF16),
            pltpu.VMEM((K, NY, 1, 128), F32),
            pltpu.VMEM((K, NY, T, SUB), BF16),
            pltpu.VMEM((K, NZ, T, COL), BF16),
            pltpu.VMEM((K, NZ, T, COL), BF16),
            pltpu.VMEM((K, T, COL), BF16),
            pltpu.VMEM((SENT, LEN, 128), F32),
            pltpu.VMEM((2, SENT // 2, COL), F32),
            pltpu.VMEM((NZ, SENT, 128), F32),
            pltpu.VMEM((NY, SENT, 128), F32),
            pltpu.VMEM((NY, SENT // NY, 128), F32),
            dma((2,)),
            dma((5,)),
            dma((3,)),
            dma((3,)),
            dma((NZ, 2 * PARTS)),
            dma((K, NZ)),
            dma((K, NY)),
            dma((K, NY)),
            dma((K, NY)),
            dma((K, NY)),
            dma((K, NY)),
            dma((K, NY)),
            dma((K, NZ)),
            dma((K, NZ)),
            dma((K, NZ)),
            dma((NY,)),
            dma((NY,)),
            dma,
            dma,
            dma((NZ,)),
            dma((NZ,)),
            dma((NY,)),
            dma((NY,)),
        ],
        compiler_params=pltpu.CompilerParams(
            collective_id=0, has_side_effects=True, vmem_limit_bytes=40 * 1024 * 1024
        ),
    )(hidden_in, norm_gain, gate_weight, up_weight, down, lengths)


def solution(mesh):
    placed = (
        P("dp", "tensor"),
        P("section", None),
        P("section", "dp", "tensor"),
        P("section", "dp", "tensor"),
        P("section", "dp", "tensor"),
        P("dp"),
    )
    return jax.shard_map(
        per_device, mesh=mesh, in_specs=placed, out_specs=P("section", "dp", None), check_vma=False
    )
```
